128 devices in a mesh: row: 16 (over y, x), col: 8 (over z, core).
Axes of the slice: x: 4, y: 4, z: 4, core: 2. Of those that a mesh axis runs over, the one named last changes fastest.
Arguments:
- features: bfloat16 [65536, 512], P('col', 'row'), may hold values from -6 to 6
- weight_t: bfloat16 [512, 512], P(None, 'row'), may hold values from -0.25 to 0.25
- tiles: bfloat16 [32768, 128, 128], P(('row', 'col')), may hold values from -0.109375 to 0.109375
- coords: int32 [2, 32768], P(None, ('row', 'col')), may hold values from 0 to 63, as said below
- counts: int32 [128], P(('row', 'col')), may hold values from 32 to 256, as said below
Outputs:
- output: bfloat16 [65536, 512], P('row', 'col')
The draws below stay inside these ranges and needn't reach their ends.
Inputs may be any that keep to these rules, and one draw needn't show every extreme that they name: coords[0] of a slot lies in 0 to 31 and coords[1] in 0 to 63; the live slots of one grid cell name distinct tiles. `counts`: some grid cell has all 256 slots live in every draw.
All inputs are finite; a program needn't handle non-finite values.
Results may differ from the reference program's by a relative error of at most 0.0095.
Values may be sent and summed in bfloat16 or wider, within the bound.
A program may use at most 128 MiB of HBM per device.

```python
import jax
import jax.numpy as jnp
from jax import lax

TILE = 128
FEAT = 512
F_OUT = 512
TROW = 32
MAXT = 256
TCOL = 64
NODES = 65536
N_COL = 8
DEVICES = 128


def draw_coords(key, part):
    keys = jax.random.split(jax.random.fold_in(key, 11), DEVICES)
    spots = jax.vmap(lambda k: jax.random.permutation(k, TROW * TCOL)[:MAXT])(keys)
    spots = spots.reshape(DEVICES * MAXT).astype(jnp.int32)
    return jnp.stack([spots // TCOL, spots % TCOL]).astype(jnp.int32)


def draw_counts(key, part):
    base = jax.random.randint(jax.random.fold_in(key, 21), (DEVICES,), MAXT // 8, MAXT // 2 + 1)
    heavy = jax.random.randint(jax.random.fold_in(key, 22), (DEVICES,), 0, 8) == 0
    chosen = jax.random.randint(jax.random.fold_in(key, 23), (), 0, DEVICES)
    heavy = heavy | (jnp.arange(DEVICES, dtype=jnp.int32) == chosen)
    return jnp.where(heavy, MAXT, base).astype(jnp.int32)


def level_of(key, shape, cuts, least, high):
    level, own = 1.0, jax.random.fold_in(key, 6)
    for axis_at, parts in cuts:
        heights = jnp.exp(jax.random.uniform(jax.random.fold_in(own, axis_at), (parts,), jnp.float32, least / len(cuts), high / len(cuts)))
        level = level * jnp.repeat(heights, shape[axis_at] // parts).reshape([-1 if axis == axis_at else 1 for axis in range(len(shape))])
    return level


def scatter_about(key, dims, deviation, limit, pieces=(), kind=jnp.bfloat16):
    values = deviation * jax.random.normal(key, dims, jnp.float32)
    if pieces:
        values = values * level_of(key, dims, pieces, -0.22, 0.18)
    return jnp.clip(values, -limit, limit).astype(kind)


def setup_inputs(seed: int = 0) -> dict:
    streams_of = jax.random.split(jax.random.key(seed), 6)
    return {
        "features": scatter_about(streams_of[0], (NODES, FEAT), 1.0, 6.0, ((0, 8), (1, 16))),
        "weight_t": scatter_about(streams_of[1], (F_OUT, FEAT), FEAT ** -0.5, 0.25, ((1, 16),)),
        "tiles": scatter_about(streams_of[2], (DEVICES * MAXT, TILE, TILE), (2 * MAXT * TILE * N_COL // (5 * TROW)) ** -0.5, 0.109375, ((0, 128),)),
        "coords": draw_coords(jax.random.fold_in(streams_of[5], 71), 0),
        "counts": draw_counts(jax.random.fold_in(streams_of[5], 71), 0),
    }


def reference(features, weight_t, tiles, coords, counts):
    feat = features.shape[1]
    cblock = TCOL * TILE
    rblock = TROW * TILE
    lanes = jnp.arange(TROW, dtype=jnp.int32)
    slots = jnp.arange(MAXT, dtype=jnp.int32)

    def device(total, cell):
        rpos = cell // N_COL
        cpos = cell % N_COL
        block = lax.dynamic_slice_in_dim(tiles, (cell * MAXT).astype(jnp.int32), MAXT, 0).astype(jnp.float32)
        place = lax.dynamic_slice_in_dim(coords, (cell * MAXT).astype(jnp.int32), MAXT, 1)
        live = (slots < counts[cell]).astype(jnp.float32)
        panel = lax.dynamic_slice_in_dim(features, (cpos * cblock).astype(jnp.int32), cblock, 0)
        panel = panel.astype(jnp.float32).reshape(TCOL, TILE, feat)
        picked = panel[place[1]]
        prod = jnp.einsum('gij,gjw->giw', block * live[:, None, None], picked, precision=lax.Precision.HIGHEST)
        select = (place[0][:, None] == lanes[None, :]).astype(jnp.float32)
        part = jnp.einsum('gt,giw->tiw', select, prod, precision=lax.Precision.HIGHEST).reshape(rblock, feat)
        start = (rpos * rblock).astype(jnp.int32)
        old = lax.dynamic_slice_in_dim(total, start, rblock, 0)
        return lax.dynamic_update_slice_in_dim(total, old + part, start, 0), None

    total = jnp.zeros((NODES, feat), jnp.float32)
    total, _ = lax.scan(device, total, jnp.arange(DEVICES, dtype=jnp.int32))
    result = jnp.dot(total, weight_t.astype(jnp.float32).T, precision=lax.Precision.HIGHEST)
    return result.astype(jnp.bfloat16)
```

```python
import functools

import jax
import jax.numpy as jnp
from jax import lax
from jax.experimental import pallas as pl
from jax.experimental.pallas import tpu as pltpu
from jax.sharding import PartitionSpec as P

MESH = pl.DeviceIdType.MESH
SLOTS = 256
TROW = 32
PAIRS = 144
NODES_IN = 8192
F_OUT = 512
LANES = NODES_IN + F_OUT
HALF = LANES // 2
UNROLL = 8
BF16 = jnp.bfloat16
F32 = jnp.float32


def as_column(row):
    half = jnp.transpose(jnp.broadcast_to(row, (128, SLOTS)))
    return jnp.concatenate([half, half], axis=1)


def slot_order(rows, cols, count):
    slot = lax.broadcasted_iota(jnp.int32, (1, SLOTS), 1)
    live = slot < count
    rows = jnp.where(live, rows, 64)
    rows_c = as_column(rows)
    line = lax.broadcasted_iota(jnp.int32, (SLOTS, SLOTS), 0)
    lane = lax.broadcasted_iota(jnp.int32, (SLOTS, SLOTS), 1)
    rank = jnp.sum(jnp.where((rows_c == rows) & (line < lane), 1, 0), axis=0, keepdims=True)
    rank_c = as_column(rank)
    base = jnp.sum(jnp.where((rows_c < rows) & ((rank_c & 1) == 0), 1, 0), axis=0, keepdims=True)
    place = jnp.where(live, 2 * base + rank, 1 << 20)
    place_c = as_column(place)
    code = slot * 128 + cols * 2 + jnp.where(rank == 0, 0, 1)
    code_c = as_column(code)
    codes = []
    for block in range(3):
        spot = lax.broadcasted_iota(jnp.int32, (SLOTS, 128), 1) + block * 128
        here = place_c[:, :128] == spot
        found = jnp.sum(jnp.where(here, code_c[:, :128] + 1, 0), axis=0, keepdims=True)
        codes.append(jnp.where(found == 0, SLOTS * 128, found - 1))
    row_lane = lax.broadcasted_iota(jnp.int32, (SLOTS, 128), 1)
    last = jnp.max(
        jnp.where(rows_c[:, :128] == row_lane, place_c[:, :128] >> 1, -1), axis=0, keepdims=True
    )
    last = jnp.where(last < 0, PAIRS, last)
    return jnp.concatenate(codes, axis=1), last


def kernel(
    feat, weight, tiles, coords, count, out,
    f0, f1, f2, f3, turned, run, meta_v, meta_s, dsend, drecv, zsend, zrecv, own, total, osend,
    local_sem, p1_send, p1_recv, p2_send, p2_recv, d_send, d_recv, z_send, z_recv, o_send, o_recv,
):
    groups = (f0, f1, f2, f3)
    row, col = lax.axis_index("row"), lax.axis_index("col")
    y, x = row // 4, row % 4
    z, core = col // 2, col % 2

    def at_x(step):
        return (y * 4 + (x + step + 4) % 4, col)

    def at_y(step):
        return (((y + step + 4) % 4) * 4 + x, col)

    def at_col(dz, other):
        k = 1 - core if other else core
        return (row, ((z + dz) % 4) * 2 + k)

    def remote(src, dst, send, recv, device):
        return pltpu.make_async_remote_copy(
            src_ref=src, dst_ref=dst, send_sem=send, recv_sem=recv, device_id=device, device_id_type=MESH
        )

    loads = []
    for q in range(2):
        lines = pl.ds(q * 16, 16)
        into = pl.ds(q * 64, 16)
        loads.append((feat.at[lines], f0.at[into, pl.ds(0, NODES_IN)]))
        loads.append((weight.at[lines], f0.at[into, pl.ds(NODES_IN, F_OUT)]))
    loads.append((tiles, turned.at[pl.ds(0, SLOTS)]))
    loads = [pltpu.make_async_copy(a, b, local_sem.at[n]) for n, (a, b) in enumerate(loads)]
    for load in loads:
        load.start()

    barrier = pltpu.get_barrier_semaphore()
    peers = [at_x(1), at_x(-1), at_y(1), at_y(-1)]
    others = [(dz, o) for dz in range(4) for o in (0, 1) if (dz, o) != (0, 0)]
    peers += [at_col(dz, o) for dz, o in others]
    for peer in peers:
        pl.semaphore_signal(barrier, inc=1, device_id=peer, device_id_type=MESH)
    for load in loads[:4]:
        load.wait()
    pl.semaphore_wait(barrier, len(peers))

    def lanes(h):
        return pl.ds(h * HALF, HALF)

    def neighbour(q, d, phase):
        step = 1 if d == 0 else -1
        return at_x(step) if (q == 0) == (phase == 1) else at_y(step)

    phase1 = {}
    for step in range(3):
        for q in range(2):
            for d in range(2):
                h = (d, 1 - d, d)[step]
                src = (0, 0, 32 if d == 0 else 16)[step]
                dst = (32 if d == 0 else 16, 32 if d == 0 else 16, 48)[step]
                n = (q * 2 + d) * 3 + step
                phase1[q, d, step] = remote(
                    f0.at[pl.ds(64 * q + src, 16), lanes(h)],
                    f0.at[pl.ds(64 * q + dst, 16), lanes(h)],
                    p1_send.at[n], p1_recv.at[n], neighbour(q, d, 1),
                )
    for step in range(2):
        for q in range(2):
            for d in range(2):
                phase1[q, d, step].start()

    phase2 = {}
    for g in (1, 2, 3):
        for q in range(2):
            for b in range(4):
                d = int((b >= 2) == (g != 2))
                lines = pl.ds(64 * q + 16 * b, 16)
                src = f0 if g < 3 else f1
                n = ((g - 1) * 2 + q) * 4 + b
                phase2[g, q, b] = remote(
                    src.at[lines], groups[g].at[lines], p2_send.at[n], p2_recv.at[n], neighbour(q, d, 2)
                )

    codes, last = slot_order(coords[0:1, :], coords[1:2, :], count[0])
    meta_v[0:1, 0:384] = codes
    meta_v[1:2, 0:128] = last
    to_smem = pltpu.make_async_copy(meta_v, meta_s, local_sem.at[5])
    to_smem.start()

    run[PAIRS] = jnp.zeros((128, 128), F32)
    loads[4].wait()
    turned[SLOTS] = jnp.zeros((128, 128), BF16)

    def turn(lo, hi):
        def step(n, carry):
            for u in range(4):
                turned[lo + n * 4 + u] = jnp.transpose(turned[lo + n * 4 + u])
            return carry

        lax.fori_loop(0, (hi - lo) // 4, step, 0)

    turn(0, 64)
    for q in range(2):
        for d in range(2):
            phase1[q, d, 0].wait_recv()
            phase1[q, d, 2].start()
    for q in range(2):
        phase2[1, q, 0].start()
    turn(64, 160)
    for q in range(2):
        for d in range(2):
            phase1[q, d, 1].wait_recv()
    for q in range(2):
        phase2[1, q, 1].start()
        phase2[1, q, 2].start()
        phase2[2, q, 2].start()
    turn(160, 256)
    to_smem.wait()
    for q in range(2):
        for d in range(2):
            phase1[q, d, 2].wait_recv()
    for q in range(2):
        phase2[1, q, 3].start()
        phase2[2, q, 3].start()
        phase2[2, q, 0].start()
        phase2[2, q, 1].start()

    def apply(group):
        def step(n, acc):
            for u in range(UNROLL):
                p = n * UNROLL + u
                one = meta_s[0, 2 * p]
                two = meta_s[0, 2 * p + 1]
                lane1 = ((one >> 1) & 63) * 128
                lane2 = ((two >> 1) & 63) * 128
                left = jnp.concatenate([group[:, pl.ds(lane1, 128)], group[:, pl.ds(lane2, 128)]], axis=1)
                right = jnp.concatenate([turned[one >> 7], turned[two >> 7]], axis=0)
                prod = jnp.dot(left, right, preferred_element_type=F32)
                acc = acc * (one & 1).astype(F32) + prod
                run[p] = acc
            return acc

        lax.fori_loop(0, PAIRS // UNROLL, step, jnp.zeros((128, 128), F32))

    def to_pair(g):
        copy = remote(dsend.at[g], drecv.at[g], d_send.at[g], d_recv.at[g], at_col(0, 1))
        for dz in range(4):
            to = ((z + dz) % 4) * 2 + (1 - core)
            for u in range(4):
                dsend[g, dz, :, u * 128 : (u + 1) * 128] = run[meta_s[1, to * 4 + u]].astype(BF16)
        copy.start()
        return copy

    def to_planes(g, pair):
        pair.wait_recv()
        copies = []
        for dz in (1, 3, 2, 0):
            to = ((z + dz) % 4) * 2 + core
            for u in range(4):
                part = slice(u * 128, (u + 1) * 128)
                both = run[meta_s[1, to * 4 + u]] + drecv[g, dz, :, part].astype(F32)
                if dz:
                    zsend[g, dz - 1, :, part] = both.astype(BF16)
                else:
                    own[g, :, part] = both
            if dz:
                n = g * 3 + dz - 1
                copy = remote(zsend.at[g, dz - 1], zrecv.at[g, dz - 1], z_send.at[n], z_recv.at[n], at_col(dz, 0))
                copy.start()
                copies.append(copy)
        return copies

    def finish(g, copies):
        for copy in copies:
            copy.wait_recv()
        spread = own[g]
        for k in range(3):
            spread = spread + zrecv[g, k].astype(F32)
        part = lax.dot_general(
            groups[g][:, NODES_IN:LANES], spread.astype(BF16), (((0,), (0,)), ((), ())), preferred_element_type=F32
        )
        if g == 0:
            total[...] = part
        else:
            total[...] += part

    pairs, planes = {}, {}
    for g in range(4):
        if g == 1:
            for b in (0, 2, 1, 3):
                for q in range(2):
                    phase2[1, q, b].wait_recv()
                    phase2[3, q, b].start()
        elif g > 1:
            for q in range(2):
                for b in range(4):
                    phase2[g, q, b].wait_recv()
        apply(groups[g])
        pairs[g] = to_pair(g)
        if g:
            finish(g - 1, planes[g - 1])
        planes[g] = to_planes(g, pairs[g])
    finish(3, planes[3])

    outs = []
    for dz, o in [(1, 0), (1, 1), (3, 0), (3, 1), (2, 0), (2, 1), (0, 1)]:
        k = 1 - core if o else core
        to = ((z + dz) % 4) * 2 + k
        n = dz * 2 + o
        osend[n] = total[pl.ds(pl.multiple_of(to * 64, 64), 64), :].astype(BF16)
        copy = remote(
            osend.at[n], out.at[:, pl.ds(pl.multiple_of(col * 512, 512), 512)], o_send.at[n], o_recv.at[n], at_col(dz, o)
        )
        copy.start()
        outs.append(copy)
    out[:, pl.ds(pl.multiple_of(col * 512, 512), 512)] = total[pl.ds(pl.multiple_of(col * 64, 64), 64), :].astype(BF16)

    for copy in list(phase1.values()) + list(phase2.values()) + list(pairs.values()):
        copy.wait_send()
    for g in range(4):
        for copy in planes[g]:
            copy.wait_send()
    for copy in outs:
        copy.wait()


def body(features, weight_t, tiles, coords, counts):
    vmem = pl.BlockSpec(memory_space=pltpu.VMEM)
    anywhere = pl.BlockSpec(memory_space=pl.ANY)
    dma = pltpu.SemaphoreType.DMA
    out = pl.pallas_call(
        kernel,
        out_shape=jax.ShapeDtypeStruct((64, 4096), BF16),
        in_specs=[anywhere, anywhere, anywhere, vmem, pl.BlockSpec(memory_space=pltpu.SMEM)],
        out_specs=vmem,
        scratch_shapes=[
            *[pltpu.VMEM((128, LANES), BF16) for _ in range(4)],
            pltpu.VMEM((SLOTS + 1, 128, 128), BF16),
            pltpu.VMEM((PAIRS + 1, 128, 128), F32),
            pltpu.VMEM((8, 512), jnp.int32),
            pltpu.SMEM((8, 512), jnp.int32),
            pltpu.VMEM((4, 4, 128, 512), BF16),
            pltpu.VMEM((4, 4, 128, 512), BF16),
            pltpu.VMEM((4, 3, 128, 512), BF16),
            pltpu.VMEM((4, 3, 128, 512), BF16),
            pltpu.VMEM((4, 128, 512), F32),
            pltpu.VMEM((512, 512), F32),
            pltpu.VMEM((8, 64, 512), BF16),
            dma((6,)), dma((12,)), dma((12,)), dma((24,)), dma((24,)), dma((4,)), dma((4,)),
            dma((12,)), dma((12,)), dma((8,)), dma((8,)),
        ],
        compiler_params=pltpu.CompilerParams(
            collective_id=0, has_side_effects=True, vmem_limit_bytes=60 * 1024 * 1024
        ),
    )(features.T, weight_t.T, tiles, coords, counts)
    return out.T


def solution(mesh):
    placed = (
        P("col", "row"),
        P(None, "row"),
        P(("row", "col"), None, None),
        P(None, ("row", "col")),
        P(("row", "col")),
    )
    return jax.shard_map(
        body, mesh=mesh, in_specs=placed, out_specs=P("row", "col"), check_vma=False
    )
```

```python
import functools

import jax
import jax.numpy as jnp
from jax import lax
from jax.experimental import pallas as pl
from jax.experimental.pallas import tpu as pltpu
from jax.sharding import PartitionSpec as P

MESH = pl.DeviceIdType.MESH
SLOTS = 256
TROW = 32
PAIRS = 144
NODES_IN = 8192
O_PART = 128
LANES = NODES_IN + O_PART
HALF = 4096
UNROLL = 48
BF16 = jnp.bfloat16
F32 = jnp.float32


def phase(name):
    return jax.named_scope(name)


def as_column(row):
    half = jnp.transpose(jnp.broadcast_to(row, (128, SLOTS)))
    return jnp.concatenate([half, half], axis=1)


def slot_order(rows, cols, count):
    slot = lax.broadcasted_iota(jnp.int32, (1, SLOTS), 1)
    live = slot < count
    rows = jnp.where(live, rows, 64)
    rows_c = as_column(rows)
    line = lax.broadcasted_iota(jnp.int32, (SLOTS, SLOTS), 0)
    lane = lax.broadcasted_iota(jnp.int32, (SLOTS, SLOTS), 1)
    rank = jnp.sum(jnp.where((rows_c == rows) & (line < lane), 1, 0), axis=0, keepdims=True)
    rank_c = as_column(rank)
    base = jnp.sum(jnp.where((rows_c < rows) & ((rank_c & 1) == 0), 1, 0), axis=0, keepdims=True)
    place = jnp.where(live, 2 * base + rank, 1 << 20)
    place_c = as_column(place)
    code = slot * 128 + cols * 2 + jnp.where(rank == 0, 0, 1)
    code_c = as_column(code)
    codes = []
    for block in range(3):
        spot = lax.broadcasted_iota(jnp.int32, (SLOTS, 128), 1) + block * 128
        here = place_c[:, :128] == spot
        found = jnp.sum(jnp.where(here, code_c[:, :128] + 1, 0), axis=0, keepdims=True)
        codes.append(jnp.where(found == 0, SLOTS * 128, found - 1))
    row_lane = lax.broadcasted_iota(jnp.int32, (SLOTS, 128), 1)
    last = jnp.max(
        jnp.where(rows_c[:, :128] == row_lane, place_c[:, :128] >> 1, -1), axis=0, keepdims=True
    )
    last = jnp.where(last < 0, PAIRS, last)
    return jnp.concatenate(codes, axis=1), last


def kernel(
    feat, weight, tiles, coords, counts, out,
    f0, f1, f2, f3, f4, turned, run, places, count, meta_v, meta_s,
    dsend, drecv, zsend, zrecv, own, wparts, total, osend,
    local_sem, p1_send, p1_recv, p2_send, p2_recv, w_send, w_recv,
    d_send, d_recv, z_send, z_recv, o_send, o_recv,
):
    groups = (f0, f1, f2, f3, f4)
    depth = [group.shape[0] for group in groups]
    row, col = lax.axis_index("row"), lax.axis_index("col")
    y, x = row // 4, row % 4
    z, core = col // 2, col % 2

    def at_x(step):
        return (y * 4 + (x + step + 4) % 4, col)

    def at_y(step):
        return (((y + step + 4) % 4) * 4 + x, col)

    def at_col(dz, other):
        k = 1 - core if other else core
        return (row, ((z + dz) % 4) * 2 + k)

    def remote(src, dst, send, recv, device):
        return pltpu.make_async_remote_copy(
            src_ref=src, dst_ref=dst, send_sem=send, recv_sem=recv, device_id=device, device_id_type=MESH
        )

    barrier = pltpu.get_barrier_semaphore()
    peers = [at_col(dz, o) for dz in (2, 1, 3, 0) for o in (0, 1) if (dz, o) != (0, 0)]
    peers = peers[:6] + [at_x(1), at_x(-1), at_y(1), at_y(-1)] + peers[6:]
    for peer in peers:
        pl.semaphore_signal(barrier, inc=1, device_id=peer, device_id_type=MESH)

    loads = []
    for q in range(2):
        lines = pl.ds(q * 16, 16)
        into = pl.ds(q * 64, 16)
        loads.append((feat.at[lines], f0.at[into, pl.ds(0, NODES_IN)]))
        part = pl.ds(pl.multiple_of(z * O_PART, O_PART), O_PART)
        loads.append((weight.at[lines, part], f0.at[into, pl.ds(NODES_IN, O_PART)]))
    loads += [(coords, places), (counts, count)]
    loads.append((tiles, turned.at[pl.ds(0, SLOTS)]))
    loads = [pltpu.make_async_copy(a, b, local_sem.at[n]) for n, (a, b) in enumerate(loads)]
    for load in loads:
        load.start()
    with phase("loads"):
        for load in loads[:4]:
            load.wait()
    with phase("barrier"):
        pl.semaphore_wait(barrier, len(peers))

    def lanes(h):
        return pl.ds(h * HALF, HALF if h == 0 else LANES - HALF)

    def neighbour(q, d, phase):
        step = 1 if d == 0 else -1
        return at_x(step) if (q == 0) == (phase == 1) else at_y(step)

    both = [(q, d) for q in range(2) for d in range(2)]
    phase1 = {}
    for step in range(3):
        for q, d in both:
            h = (d, 1 - d, d)[step]
            src = (0, 0, 32 if d == 0 else 16)[step]
            dst = (32 if d == 0 else 16, 32 if d == 0 else 16, 48)[step]
            n = (q * 2 + d) * 3 + step
            phase1[q, d, step] = remote(
                f0.at[pl.ds(64 * q + src, 16), lanes(h)],
                f0.at[pl.ds(64 * q + dst, 16), lanes(h)],
                p1_send.at[n], p1_recv.at[n], neighbour(q, d, 1),
            )

    phase2 = {}
    for q, d in both:
        for k in range(6):
            if k < 4:
                src, line = f0, 64 * q + 16 * k
                dst, to = (f1, f2)[k // 2], 64 * q + 32 * d + 16 * (k % 2)
            else:
                src, line = (f1, f2)[d], 64 * q + 32 * d + 16 * (k - 4)
                dst, to = (f3, f4)[k - 4], 32 * q + 16 * d
            n = (q * 2 + d) * 6 + k
            phase2[q, d, k] = remote(
                src.at[pl.ds(line, 16)], dst.at[pl.ds(to, 16)], p2_send.at[n], p2_recv.at[n], neighbour(q, d, 2)
            )

    for step in range(2):
        for q, d in both:
            phase1[q, d, step].start()
    for q, d in both:
        phase2[q, d, 0].start()

    loads[4].wait()
    loads[5].wait()
    with phase("order"):
        codes, last = slot_order(places[0:1, :], places[1:2, :], count[0])
        meta_v[0:1, 0:384] = codes
        meta_v[1:2, 0:128] = last
    to_smem = pltpu.make_async_copy(meta_v, meta_s, local_sem.at[7])
    to_smem.start()

    run[PAIRS] = jnp.zeros((128, 128), F32)
    loads[6].wait()
    turned[SLOTS] = jnp.zeros((128, 128), BF16)

    def turn(lo, hi):
        def step(n, carry):
            for u in range(4):
                turned[lo + n * 4 + u] = jnp.transpose(turned[lo + n * 4 + u])
            return carry

        lax.fori_loop(0, (hi - lo) // 4, step, 0)

    with phase("turn0"):
        turn(0, 64)
    with phase("p1_0"):
        for q, d in both:
            phase1[q, d, 0].wait_recv()
            phase1[q, d, 2].start()
    with phase("turn1"):
        turn(64, 160)
    with phase("p1_1"):
        for q, d in both:
            phase1[q, d, 1].wait_recv()
        for k in (1, 2):
            for q, d in both:
                phase2[q, d, k].start()
    with phase("turn2"):
        turn(160, 256)
    to_smem.wait()
    with phase("p1_2"):
        for q, d in both:
            phase1[q, d, 2].wait_recv()
        for q, d in both:
            phase2[q, d, 3].start()

    def share_weight(g):
        lines = pl.ds(0, depth[g])
        for dz in (1, 3, 2):
            n = g * 3 + dz - 1
            copy = remote(
                groups[g].at[:, pl.ds(NODES_IN, O_PART)], wparts.at[g, dz - 1, lines],
                w_send.at[n], w_recv.at[n], at_col(dz, 0),
            )
            copy.start()
            shared.append(copy)

    shared = []

    def apply(g):
        group, lines = groups[g], depth[g]

        def step(n, acc):
            for u in range(UNROLL):
                p = n * UNROLL + u
                one = meta_s[0, 2 * p]
                two = meta_s[0, 2 * p + 1]
                lane1 = ((one >> 1) & 63) * 128
                lane2 = ((two >> 1) & 63) * 128
                left = jnp.concatenate([group[:, pl.ds(lane1, 128)], group[:, pl.ds(lane2, 128)]], axis=1)
                right = jnp.concatenate([turned[one >> 7], turned[two >> 7]], axis=0)
                prod = jnp.dot(left, right, preferred_element_type=F32)
                acc = acc * (one & 1).astype(F32) + prod
                run[p, 0:lines] = acc
            return acc

        lax.fori_loop(0, PAIRS // UNROLL, step, jnp.zeros((lines, 128), F32))

    def to_pair(g, part, parts):
        lines, n = depth[g], g + part
        share = 4 // parts
        here = pl.ds(part * share * 128, share * 128)
        copy = remote(
            dsend.at[g, :, pl.ds(0, lines), here], drecv.at[g, :, pl.ds(0, lines), here],
            d_send.at[n], d_recv.at[n], at_col(0, 1),
        )
        for dz in range(4):
            to = ((z + dz) % 4) * 2 + (1 - core)
            for u in range(part * share, (part + 1) * share):
                dsend[g, dz, 0:lines, u * 128 : (u + 1) * 128] = run[meta_s[1, to * 4 + u], 0:lines].astype(BF16)
        copy.start()
        return copy

    def to_planes(g, part, parts, pair):
        lines = depth[g]
        share = 4 // parts
        here = pl.ds(part * share * 128, share * 128)
        with phase("pair_wait"):
            pair.wait_recv()
        copies = []
        for dz in (2, 1, 3, 0):
            to = ((z + dz) % 4) * 2 + core
            for u in range(part * share, (part + 1) * share):
                at = slice(u * 128, (u + 1) * 128)
                summed = run[meta_s[1, to * 4 + u], 0:lines] + drecv[g, dz, 0:lines, at].astype(F32)
                if dz:
                    zsend[g, dz - 1, 0:lines, at] = summed.astype(BF16)
                else:
                    own[g, 0:lines, at] = summed
            if dz:
                n = (g + part) * 3 + dz - 1
                copy = remote(
                    zsend.at[g, dz - 1, pl.ds(0, lines), here], zrecv.at[g, dz - 1, pl.ds(0, lines), here],
                    z_send.at[n], z_recv.at[n], at_col(dz, 0),
                )
                copy.start()
                copies.append(copy)
        return copies

    def finish(g, part, parts, copies):
        lines = depth[g]
        width = 512 // parts
        at = slice(part * width, (part + 1) * width)
        with phase("plane_wait"):
            for copy in copies:
                copy.wait_recv()
            if part == 0:
                for copy in shared[3 * g : 3 * g + 3]:
                    copy.wait_recv()
        spread = own[g, 0:lines, at]
        for k in range(3):
            spread = spread + zrecv[g, k, 0:lines, at].astype(F32)
        spread = spread.astype(BF16)
        for dz in range(4):
            if dz:
                piece = wparts[g, dz - 1, 0:lines]
            else:
                piece = groups[g][:, NODES_IN:LANES]
            product = lax.dot_general(piece, spread, (((0,), (0,)), ((), ())), preferred_element_type=F32)
            to = pl.ds(pl.multiple_of(((z - dz + 4) % 4) * O_PART, O_PART), O_PART)
            if g == 0:
                total[to, at] = product
            else:
                total[to, at] += product

    pairs, planes = [], []

    def partial_sums(g):
        share_weight(g)
        parts = 2 if g == 4 else 1
        with phase(f"apply{g}"):
            apply(g)
        for part in range(parts):
            with phase(f"to_pair{g}"):
                pairs.append(to_pair(g, part, parts))
        for part in range(parts):
            with phase(f"to_planes{g}"):
                planes.append(to_planes(g, part, parts, pairs[g + part]))

    def done(g):
        with phase(f"finish{g}"):
            finish(g, 0, 1, planes[g])

    partial_sums(0)
    with phase("p2_1"):
        for k in (0, 1):
            for q, d in both:
                phase2[q, d, k].wait_recv()
                if d == 0:
                    phase2[q, d, k + 4].start()
    partial_sums(1)
    with phase("p2_2"):
        for k in (2, 3):
            for q, d in both[::-1]:
                phase2[q, d, k].wait_recv()
                if d == 1:
                    phase2[q, d, k + 2].start()
    partial_sums(2)
    done(0)
    with phase("p2_3"):
        for q, d in both:
            phase2[q, d, 4].wait_recv()
    partial_sums(3)
    done(1)
    with phase("p2_4"):
        for q, d in both:
            phase2[q, d, 5].wait_recv()
    partial_sums(4)
    done(2)
    done(3)

    outs = []
    for part in range(2):
        with phase(f"finish{4 + part}"):
            finish(4, part, 2, planes[4 + part])
        at = slice(part * 256, part * 256 + 256)
        here = pl.ds(pl.multiple_of(col * 512 + part * 256, 256), 256)
        for dz, o in [(2, 0), (2, 1), (1, 0), (1, 1), (3, 0), (3, 1), (0, 1)]:
            k = 1 - core if o else core
            to = ((z + dz) % 4) * 2 + k
            n = part * 8 + dz * 2 + o
            osend[n] = total[pl.ds(pl.multiple_of(to * 64, 64), 64), at].astype(BF16)
            copy = remote(osend.at[n], out.at[:, here], o_send.at[n], o_recv.at[n], at_col(dz, o))
            copy.start()
            outs.append(copy)
        out[:, here] = total[pl.ds(pl.multiple_of(col * 64, 64), 64), at].astype(BF16)

    with phase("drain"):
        for copy in list(phase1.values()) + list(phase2.values()) + pairs + sum(planes, []) + shared:
            copy.wait_send()
    with phase("out_wait"):
        for copy in outs:
            copy.wait()


def body(features, weight_t, tiles, coords, counts):
    anywhere = pl.BlockSpec(memory_space=pl.ANY)
    dma = pltpu.SemaphoreType.DMA
    out = pl.pallas_call(
        kernel,
        out_shape=jax.ShapeDtypeStruct((64, 4096), BF16),
        in_specs=[anywhere] * 5,
        out_specs=pl.BlockSpec(memory_space=pltpu.VMEM),
        scratch_shapes=[
            *[pltpu.VMEM((lines, LANES), BF16) for lines in (128, 128, 128, 64, 64)],
            pltpu.VMEM((SLOTS + 1, 128, 128), BF16),
            pltpu.VMEM((PAIRS + 1, 128, 128), F32),
            pltpu.VMEM((2, SLOTS), jnp.int32),
            pltpu.SMEM((1,), jnp.int32),
            pltpu.VMEM((8, 512), jnp.int32),
            pltpu.SMEM((8, 512), jnp.int32),
            pltpu.VMEM((5, 4, 128, 512), BF16),
            pltpu.VMEM((5, 4, 128, 512), BF16),
            pltpu.VMEM((5, 3, 128, 512), BF16),
            pltpu.VMEM((5, 3, 128, 512), BF16),
            pltpu.VMEM((5, 128, 512), F32),
            pltpu.VMEM((5, 3, 128, O_PART), BF16),
            pltpu.VMEM((512, 512), F32),
            pltpu.VMEM((16, 64, 256), BF16),
            dma((8,)), dma((12,)), dma((12,)), dma((24,)), dma((24,)), dma((15,)), dma((15,)),
            dma((6,)), dma((6,)), dma((18,)), dma((18,)), dma((16,)), dma((16,)),
        ],
        compiler_params=pltpu.CompilerParams(
            collective_id=0, has_side_effects=True, vmem_limit_bytes=60 * 1024 * 1024
        ),
    )(features.T, weight_t.T, tiles, coords, counts)
    return out.T


def solution(mesh):
    placed = (
        P("col", "row"),
        P(None, "row"),
        P(("row", "col"), None, None),
        P(None, ("row", "col")),
        P(("row", "col")),
    )
    return jax.shard_map(
        body, mesh=mesh, in_specs=placed, out_specs=P("row", "col"), check_vma=False
    )
```
